32 devices in a mesh: seq: 8 (over y, x, core), dp: 4 (over z).
Axes of the slice: x: 2, y: 2, z: 4, core: 2. Of those that a mesh axis runs over, the one named last changes fastest.
Arguments:
- layer_input: bfloat16 [4, 2048, 2560], P('dp', 'seq'), may hold values from -14400 to 14400
- scan_input: bfloat16 [4, 2048, 2560], P('dp', 'seq'), may hold values from -0.75 to 0.75
- scan_cotangent: bfloat16 [4, 2048, 2560], P('dp', 'seq'), may hold values from -0.0625 to 0.0625
- step_size: float32 [4, 40, 2048], P('dp', None, 'seq'), may hold values from 0.5 to 2
- log_decay: float32 [4, 40, 2048], P('dp', None, 'seq'), may hold values from -2.25 to 0
- state_inputs: bfloat16 [4, 2048, 256], P('dp', 'seq'), may hold values from -4 to 4
- entry_state: bfloat16 [4, 8, 2560, 128], P('dp', 'seq'), may hold values from -8 to 8
Outputs:
- state_input_grad: bfloat16 [4, 2048, 256], P('dp', 'seq')
- weight_grad: float32 [2560, 256], P(('seq', 'dp'))
The draws below stay inside these ranges and needn't reach their ends.
All inputs are finite; a program needn't handle non-finite values. Where the reference program divides by a largest or mean magnitude, that divisor is 1e-20 or more.
Results may differ from the reference program's by a relative error of at most 0.013.
Values may be sent and summed in bfloat16 or wider, within the bound.
A program may use at most 128 MiB of HBM per device.

```python
import math
import jax
import jax.numpy as jnp
from jax import lax

D = 2560
HEADS = 40
HEADP = 64
NSTATE = 128
STRETCH = 256
STRETCHES_DEV = 1
TOK_DEV = 256
LSEQ = 2048
SEQS = 4
CHANNELS = 2560
N_SEQ = 8
N_DP = 4


def draw_layer_input(key, part):
    keys = jax.random.split(key, 5)
    noise_part = jax.random.truncated_normal(keys[1], -4.0, 4.0, (SEQS, LSEQ, D), jnp.float32)
    row_top = 10.0
    element_offset = lax.broadcasted_iota(jnp.float32, (1, LSEQ, 1), 1) / LSEQ
    sequence = lax.broadcasted_iota(jnp.float32, (SEQS, 1, 1), 0) / max(SEQS - 1, 1)
    row_ramp = (1.0 + 2.0 * element_offset) * (1.0 + 2.0 * sequence)
    row_scale = jnp.exp(jax.random.uniform(keys[2], (SEQS, LSEQ, 1), jnp.float32, 0.0, jnp.log(row_top)))
    column_scale = jnp.exp(jax.random.uniform(keys[3], (1, 1, D), jnp.float32, 0.0, jnp.log(10.0)))
    owners = jax.random.permutation(keys[4], N_SEQ * N_DP)
    seq_index = lax.broadcasted_iota(jnp.int32, (SEQS, LSEQ), 1) // TOK_DEV
    group_index = lax.broadcasted_iota(jnp.int32, (SEQS, LSEQ), 0)
    target = owners[seq_index * N_DP + group_index]
    column_block = lax.broadcasted_iota(jnp.int32, (1, 1, D), 2) // (D // (N_SEQ * N_DP))
    spike = jnp.where(column_block == target[:, :, None], 4.0, 1.0)
    return (noise_part * row_ramp * row_scale * column_scale * spike).astype(jnp.bfloat16)


def draw_log_decay(key, part):
    keys = jax.random.split(key, 7)
    fast_share = 0.5
    quick = jax.random.uniform(keys[0], (1, HEADS, 1), jnp.float32) < fast_share
    fast_rate = jnp.exp(jax.random.uniform(keys[1], (1, HEADS, 1), jnp.float32, jnp.log(1.0 / 50.0), jnp.log(1.0 / 30.0)))
    slow_rate = jnp.exp(jax.random.uniform(keys[2], (1, HEADS, 1), jnp.float32, jnp.log(0.05), jnp.log(0.4))) / LSEQ
    forgetting_speeds = jnp.where(quick, fast_rate, slow_rate)
    accelerator_gain = jnp.exp(jax.random.uniform(keys[3], (SEQS, HEADS, N_SEQ), jnp.float32, jnp.log(0.5), jnp.log(2.0)))
    accelerator_gain = jnp.repeat(accelerator_gain, TOK_DEV, axis=2)
    element_gain = jnp.exp(jax.random.uniform(keys[4], (SEQS, HEADS, LSEQ), jnp.float32, jnp.log(0.5), jnp.log(2.0)))
    outlier_indices = jax.random.randint(keys[5], (SEQS, 1, 1, 3), 0, LSEQ)
    objective_numbers = jax.random.uniform(keys[6], (SEQS, HEADS, 1, 3), jnp.float32, jnp.log(0.5), jnp.log(0.8))
    element_offset = lax.broadcasted_iota(jnp.int32, (1, 1, LSEQ, 1), 2)
    outlier_clusters = jnp.sum(jnp.where(element_offset == outlier_indices, objective_numbers, 0.0), axis=3)
    return -(forgetting_speeds * accelerator_gain * element_gain) + outlier_clusters


def shard_levels(rng, dims, cuts, least, high):
    gain = 1.0
    for axis_at, blocks in cuts:
        heights = jax.random.uniform(jax.random.fold_in(jax.random.fold_in(rng, 6), axis_at), (blocks,), jnp.float32, least / len(cuts), high / len(cuts))
        gain = gain * jnp.repeat(jnp.exp(heights), dims[axis_at] // blocks).reshape((-1,) + (1,) * (len(dims) - 1 - axis_at))
    return gain


def gaussian(own_key, shape, scale, bound, shards=(), held_as=jnp.bfloat16):
    values = scale * jax.random.normal(own_key, shape, jnp.float32)
    if shards:
        values = values * shard_levels(own_key, shape, shards, -0.22, 0.18)
    return jnp.clip(values, -bound, bound).astype(held_as)


def setup_inputs(seed: int = 0) -> dict:
    seeds = jax.random.split(jax.random.key(seed), 8)
    return {
        "layer_input": draw_layer_input(jax.random.fold_in(seeds[7], 71), 0),
        "scan_input": gaussian(seeds[1], (SEQS, LSEQ, CHANNELS), HEADP ** -0.5, 0.75, ((0, 4), (1, 8))),
        "scan_cotangent": gaussian(seeds[2], (SEQS, LSEQ, CHANNELS), (TOK_DEV * N_SEQ * HEADS // 8) ** -0.5, 0.0625, ((0, 4), (1, 8))),
        "step_size": jnp.clip(jnp.exp(math.log(2.0) - 1.3862944 * jax.random.uniform(seeds[3], (SEQS, HEADS, LSEQ), jnp.float32) ** shard_levels(seeds[3], (SEQS, HEADS, LSEQ), ((0, 4), (2, 8)), -0.2, 0.2)), 0.5, 2.0),
        "log_decay": draw_log_decay(jax.random.fold_in(seeds[7], 71), 0),
        "state_inputs": gaussian(seeds[5], (SEQS, LSEQ, 2 * NSTATE), 1.0, 4.0, ((0, 4), (1, 8))),
        "entry_state": gaussian(seeds[6], (SEQS, N_SEQ, CHANNELS, NSTATE), 2.0, 8.0, ((0, 4), (1, 8))),
    }


epsilon = 1e-6


def silu_slope(value):
    sigma = jax.nn.sigmoid(value)
    return sigma * (1.0 + value * (1.0 - sigma))


def block_terms(pieces):
    inputs, cotangents, steps, cumulative, writes, reads = pieces
    later = lax.broadcasted_iota(jnp.int32, (STRETCH, STRETCH), 0) >= lax.broadcasted_iota(jnp.int32, (STRETCH, STRETCH), 1)
    scores = jnp.einsum("shp,thp->hst", cotangents.astype(jnp.float32), inputs.astype(jnp.float32))
    spread = jnp.where(later[None], cumulative[:, :, None] - cumulative[:, None, :], 0.0)
    decay = jnp.where(later[None], jnp.exp(spread), 0.0)
    mixing = lax.optimization_barrier((scores * decay * steps[:, None, :]).astype(jnp.bfloat16)).astype(jnp.float32)
    inner_write = jnp.einsum("hst,sn->tn", mixing, reads.astype(jnp.float32))
    inner_read = jnp.einsum("hst,tn->sn", mixing, writes.astype(jnp.float32))
    weighted_cot = (cotangents.astype(jnp.float32) * jnp.exp(cumulative).T[:, :, None]).astype(jnp.bfloat16)
    weighted_in = (inputs.astype(jnp.float32) * (steps * jnp.exp(cumulative[:, -1:] - cumulative)).T[:, :, None]).astype(jnp.bfloat16)
    return inner_write, inner_read, weighted_cot, weighted_in, jnp.exp(cumulative[:, -1])


def rounded(state):
    return lax.optimization_barrier(state.astype(jnp.bfloat16)).astype(jnp.float32)


def backward_step(state, pieces):
    weighted, reading, cot_part, total = pieces
    carried = jnp.einsum("bthp,bhpn->btn", weighted.astype(jnp.float32), rounded(state))
    local = jnp.einsum("bthp,btn->bhpn", cot_part.astype(jnp.float32), reading.astype(jnp.float32))
    return local + total[:, :, None, None] * state, carried


def reference(layer_input, scan_input, scan_cotangent, step_size, log_decay, state_inputs, entry_state):
    blocks = LSEQ // STRETCH
    count = SEQS * blocks
    inputs = scan_input.reshape(count, STRETCH, HEADS, HEADP)
    cotangents = scan_cotangent.reshape(count, STRETCH, HEADS, HEADP)
    steps = step_size.reshape(SEQS, HEADS, blocks, STRETCH).transpose(0, 2, 1, 3).reshape(count, HEADS, STRETCH)
    decays = log_decay.reshape(SEQS, HEADS, blocks, STRETCH).transpose(0, 2, 1, 3).reshape(count, HEADS, STRETCH)
    cumulative = jnp.cumsum(decays, axis=2)
    preact = state_inputs.astype(jnp.float32)
    activated = jax.nn.silu(preact).astype(jnp.bfloat16)
    writes = activated[:, :, :NSTATE].reshape(count, STRETCH, NSTATE)
    reads = activated[:, :, NSTATE:].reshape(count, STRETCH, NSTATE)
    inner_write, inner_read, weighted_cot, weighted_in, totals = lax.map(
        block_terms, (inputs, cotangents, steps, cumulative, writes, reads))

    def by_block(array):
        return jnp.swapaxes(array.reshape((SEQS, blocks) + array.shape[1:]), 0, 1)

    ordered_in = by_block(weighted_in)
    ordered_cot = by_block(weighted_cot)
    ordered_writes = by_block(writes)
    ordered_reads = by_block(reads)
    ordered_totals = by_block(totals)
    zero_state = jnp.zeros((SEQS, HEADS, HEADP, NSTATE), jnp.float32)
    ignored, carried_write = lax.scan(backward_step, zero_state,
                                      (ordered_in, ordered_reads, ordered_cot, ordered_totals), reverse=True)

    entries = entry_state.reshape(SEQS, N_SEQ, HEADS, HEADP, NSTATE)
    block_ids = jnp.arange(blocks, dtype=jnp.int32)

    def forward_step(state, pieces):
        cot_part, writing, weighted, total, block_id = pieces
        saved = lax.dynamic_index_in_dim(entries, (block_id // STRETCHES_DEV).astype(jnp.int32), 1, keepdims=False)
        state = jnp.where(block_id % STRETCHES_DEV == 0, saved.astype(jnp.float32), state)
        carried = jnp.einsum("bthp,bhpn->btn", cot_part.astype(jnp.float32), rounded(state))
        local = jnp.einsum("bthp,btn->bhpn", weighted.astype(jnp.float32), writing.astype(jnp.float32))
        return local + total[:, :, None, None] * state, carried

    ignored, carried_read = lax.scan(forward_step, zero_state,
                                     (ordered_cot, ordered_writes, ordered_in, ordered_totals, block_ids))

    def by_token(array):
        return jnp.swapaxes(array, 0, 1).reshape(SEQS, LSEQ, NSTATE)

    grad_write = inner_write.reshape(SEQS, LSEQ, NSTATE) + by_token(carried_write)
    grad_read = inner_read.reshape(SEQS, LSEQ, NSTATE) + by_token(carried_read)
    state_input_grad = (jnp.concatenate([grad_write, grad_read], axis=2) * silu_slope(preact)).astype(jnp.bfloat16)

    peaks = jnp.max(jnp.abs(layer_input), axis=(0, 1)).astype(jnp.float32)
    factor = 1.0 / (peaks + epsilon)

    def add_sequence(running, pieces):
        rows, grads = pieces
        quantized = (rows.astype(jnp.float32) * factor).astype(jnp.bfloat16)
        product = lax.dot_general(quantized, grads, (((0,), (0,)), ((), ())), preferred_element_type=jnp.float32)
        return running + product, None

    summed, ignored = lax.scan(add_sequence, jnp.zeros((D, 2 * NSTATE), jnp.float32), (layer_input, state_input_grad))
    return state_input_grad, summed
```

```python
import functools
import math

import jax
import jax.numpy as jnp
from jax import lax
from jax.experimental import pallas as pl
from jax.experimental.pallas import tpu as pltpu
from jax.sharding import PartitionSpec as P

MESH = pl.DeviceIdType.MESH
F32 = jnp.float32
BF16 = jnp.bfloat16
LANES = 128
LOG2E = 1.4426950408889634
EPSILON = 1e-06


def nt(a, b, precision=None):
    return lax.dot_general(
        a, b, (((1,), (1,)), ((), ())), preferred_element_type=F32, precision=precision
    )


def tn(a, b):
    return lax.dot_general(a, b, (((0,), (0,)), ((), ())), preferred_element_type=F32)


def nn(a, b):
    return jnp.dot(a, b, preferred_element_type=F32)


class Sizes:
    def __init__(self, n_seq, n_dp, tokens, width, channels, heads, states):
        self.n_seq, self.n_dp, self.tokens, self.width = n_seq, n_dp, tokens, width
        self.channels, self.heads, self.states = channels, heads, states
        self.head = channels // heads
        self.bits = n_seq.bit_length() - 1
        self.half_heads = heads // 2
        self.half_pairs = channels // LANES // 2
        self.per = LANES // self.head
        self.chunks = max(c for c in range(1, 6) if self.half_pairs % c == 0)
        self.chunk_pairs = self.half_pairs // self.chunks
        self.chunk_rows = self.chunk_pairs * LANES
        self.chunk_heads = self.chunk_rows // self.head
        self.wide = width // LANES
        self.wide_pad = -(-self.wide // 16) * 16
        self.rows_seq = width // n_seq
        self.rows = self.rows_seq // n_dp


def kernel(
    z,
    layer_hbm, scan_hbm, cot_hbm, entry_hbm, step_ref, decay_ref, state_ref,
    grad_out, weight_out,
    layer, scan, cot, entry, local_sem,
    crow, ccol, wcol, wcot, win,
    fsend, frecv, fown, fhigh, fsum, bsum, dsend, drecv, beyond, bsend, brecv,
    fsem_s, fsem_r, dsem_s, dsem_r, bsem_s, bsem_r,
    mix, part, wsend, wrecv, wsem_s, wsem_r, zsend, zrecv, zown, zsem_s, zsem_r,
    peak, peak_send, peak_recv, peak_send2, peak_recv2, pkcol,
    psem_s, psem_r, qsem_s, qsem_r,
):
    n, m, t = z.n_seq, z.n_dp, z.tokens
    me, dz = lax.axis_index("seq"), lax.axis_index("dp")
    bit = [lax.rem(me // (1 << b), 2) for b in range(z.bits)]
    mate = [me + (1 - 2 * bit[b]) * (1 << b) for b in range(z.bits)]
    mine, other = bit[0], 1 - bit[0]

    locals_ = [
        pltpu.make_async_copy(src, dst, local_sem.at[i])
        for i, (src, dst) in enumerate(
            ((cot_hbm, cot), (scan_hbm, scan), (layer_hbm, layer), (entry_hbm, entry))
        )
    ]
    for c in locals_:
        c.start()

    barrier = pltpu.get_barrier_semaphore()
    for o in range(1, n):
        pl.semaphore_signal(
            barrier, inc=1, device_id={"seq": lax.rem(me + o, n), "dp": dz}, device_id_type=MESH
        )
    for o in range(1, m):
        pl.semaphore_signal(
            barrier, inc=1, device_id={"seq": me, "dp": lax.rem(dz + o, m)}, device_id_type=MESH
        )

    decay = decay_ref[...] * LOG2E
    row = lax.broadcasted_iota(jnp.int32, (t, t), 0)
    col = lax.broadcasted_iota(jnp.int32, (t, t), 1)
    lower = jnp.where(col <= row, 1.0, 0.0).astype(F32)
    high = lax.Precision.HIGHEST
    cum = nt(decay, lower, high)
    cum_t = nt(lower, decay, high)
    steps = step_ref[...]
    crow[...] = cum - jnp.log2(steps)
    weight_t = jnp.transpose(steps) * jnp.exp2(cum_t[t - 1 : t, :] - cum_t)
    lane = lax.broadcasted_iota(jnp.int32, (t, LANES), 1)
    total = jnp.broadcast_to(jnp.exp2(cum[:, t - 1 : t]), (z.heads, LANES))
    tot = [total[: z.half_heads], total[z.half_heads :]]
    tot_mine = jnp.where(mine == 1, tot[1], tot[0])
    dsend[0] = jnp.where(mine == 1, tot[0], tot[1])
    for h in range(z.heads):
        ccol[h] = jnp.broadcast_to(cum_t[:, h : h + 1], (t, LANES))

    pre = state_ref[...].astype(F32)
    sigma = 1.0 / (1.0 + jnp.exp(-pre))
    activated = (pre * sigma).astype(BF16)
    writes, reads = activated[:, : z.states], activated[:, z.states :]

    def by_head(g, table):
        value = table[g * z.per]
        for k in range(1, z.per):
            value = jnp.where(lane >= k * z.head, table[g * z.per + k], value)
        return value

    def later(g):
        at = pl.ds(pl.multiple_of(g * LANES, LANES), LANES)
        weighted = (cot[:, at].astype(F32) * jnp.exp2(by_head(g, ccol))).astype(BF16)
        wcot[:, at] = weighted
        return tn(weighted, reads)

    def remote(src, dst, s_sem, r_sem, seq, dp):
        return pltpu.make_async_remote_copy(
            src_ref=src, dst_ref=dst, send_sem=s_sem, recv_sem=r_sem,
            device_id={"seq": seq, "dp": dp}, device_id_type=MESH,
        )

    def f_copy(b, c):
        return remote(
            fsend.at[b, c], frecv.at[b, c], fsem_s.at[b, c], fsem_r.at[b, c], mate[b], dz
        )

    def d_copy(b):
        return remote(dsend.at[b], drecv.at[b], dsem_s.at[b], dsem_r.at[b], mate[b], dz)

    def spread(d, c):
        return jnp.concatenate(
            [
                jnp.broadcast_to(d[h : h + 1, :], (z.head, LANES))
                for h in range(c * z.chunk_heads, (c + 1) * z.chunk_heads)
            ],
            axis=0,
        )

    started = []

    def go(copy):
        copy.start()
        started.append(copy)
        return copy

    locals_[0].wait()
    for c in range(z.chunks):
        for p in range(z.chunk_pairs):
            g = other * z.half_pairs + c * z.chunk_pairs + p
            fsend[0, c, p * LANES : (p + 1) * LANES, :] = later(g).astype(BF16)
        if c == 0:
            pl.semaphore_wait(barrier, n - 1 + m - 1)
            go(d_copy(0))
        go(f_copy(0, c))
    for c in range(z.chunks):
        for p in range(z.chunk_pairs):
            g = mine * z.half_pairs + c * z.chunk_pairs + p
            fown[c, p * LANES : (p + 1) * LANES, :] = later(g)

    d_copy(0).wait_recv()
    tot_other = drecv[0]
    tot_low = jnp.where(mine == 1, tot_other, tot_mine)
    tot_high = jnp.where(mine == 1, tot_mine, tot_other)
    d_now = tot_low * tot_high
    if z.bits > 1:
        dsend[1] = d_now
        go(d_copy(1))
    for c in range(z.chunks):
        f_copy(0, c).wait_recv()
        own, far = fown[c], frecv[0, c].astype(F32)
        up = jnp.where(mine == 1, own, far)
        fhigh[c] = up
        value = jnp.where(mine == 1, far, own) + spread(tot_low, c) * up
        bsum[c] = jnp.zeros_like(value)
        fsum[c] = value
        if z.bits > 1:
            fsend[1, c] = value.astype(BF16)
            go(f_copy(1, c))

    locals_[2].wait()
    peak[...] = jnp.zeros_like(peak)
    for j in range(z.wide):
        block = layer[:, j * LANES : (j + 1) * LANES].astype(F32)
        peak[j : j + 1, :] = jnp.max(jnp.abs(block), axis=0, keepdims=True)
    peak_send[...] = peak[...].astype(BF16)
    peak_copies = [
        go(remote(peak_send, peak_recv.at[o - 1], psem_s.at[o - 1], psem_r.at[o - 1],
                  lax.rem(me + o, n), dz))
        for o in range(1, n)
    ]

    locals_[1].wait()
    for h in range(z.heads):
        wcol[h] = jnp.broadcast_to(weight_t[:, h : h + 1], (t, LANES))
    mix[...] = jnp.zeros_like(mix)
    hf = t // 2
    keep = row[:hf, :hf] >= col[:hf, :hf]

    def mixing(g, carry):
        at = pl.ds(pl.multiple_of(g * LANES, LANES), LANES)
        c_pair, s_pair = cot[:, at], scan[:, at]
        win[:, at] = (s_pair.astype(F32) * by_head(g, wcol)).astype(BF16)
        for k in range(z.per):
            h = g * z.per + k
            inside = (lane >= k * z.head) & (lane < (k + 1) * z.head)
            c_head = jnp.where(inside, c_pair.astype(F32), 0.0).astype(BF16)
            rows = crow[pl.ds(h, 1), :]
            for s in range(2):
                scores = nt(c_head[s * hf : (s + 1) * hf], s_pair[: (s + 1) * hf])
                for r in range(s + 1):
                    cols = ccol[h, s * hf : (s + 1) * hf, :]
                    cut = slice(r * hf, (r + 1) * hf)
                    spread_ = cols - rows[:, cut]
                    if s == r:
                        spread_ = jnp.where(keep, spread_, -1e30)
                    mix[s * hf : (s + 1) * hf, cut] += scores[:, cut] * jnp.exp2(spread_)
        return carry

    lax.fori_loop(0, z.heads // z.per, mixing, 0)

    e_now = None
    for b in range(1, z.bits):
        d_copy(b).wait_recv()
        d_far = drecv[b]
        d_low = jnp.where(bit[b] == 1, d_far, d_now)
        last = b == z.bits - 1
        if not last:
            dsend[b + 1] = d_now * d_far
            go(d_copy(b + 1))
        for c in range(z.chunks):
            f_copy(b, c).wait_recv()
            far = frecv[b, c].astype(F32)
            scaled = far if e_now is None else spread(e_now, c) * far
            gained = bsum[c] + jnp.where(bit[b] == 1, jnp.zeros_like(scaled), scaled)
            if not last:
                bsum[c] = gained
                own = fsum[c]
                value = jnp.where(bit[b] == 1, far, own) + spread(d_low, c) * jnp.where(
                    bit[b] == 1, own, far
                )
                fsum[c] = value
                fsend[b + 1, c] = value.astype(BF16)
                go(f_copy(b + 1, c))
            else:
                bsum[c] = gained
        one = jnp.ones_like(d_far) if e_now is None else e_now
        e_now = jnp.where(bit[b] == 1, one, one * d_far)
        d_now = d_now * d_far
    for o in range(1, n):
        peak_copies[o - 1].wait_recv()

    b_copies = []
    mixed = mix[...].astype(BF16)
    grad_write = tn(mixed, reads)
    for c in range(z.chunks):
        top = bsum[c]
        low = fhigh[c] + spread(tot_high, c) * top
        beyond[c] = jnp.where(mine == 1, top, low).astype(BF16)
        bsend[c] = jnp.where(mine == 1, low, top).astype(BF16)
        b_copies.append(
            go(remote(bsend.at[c], brecv.at[c], bsem_s.at[c], bsem_r.at[c], mate[0], dz))
        )

    slope = sigma * (1.0 + pre * (1.0 - sigma))
    order = {1: list(range(z.bits)), 0: [0] + list(range(1, z.bits))[::-1]}
    states = z.states

    def place(r, q):
        s = 0
        for k, b in enumerate(order[q]):
            s += ((r >> (z.bits - 1 - k)) & 1) << b
        return s

    offset = [sum(n >> (k + 1) for k in range(i)) for i in range(z.bits)]

    def w_copy(q, k):
        size = n >> (k + 1)
        at = pl.ds(offset[k], size)
        return remote(
            wsend.at[q, at], wrecv.at[q, at], wsem_s.at[q, k], wsem_r.at[q, k],
            mate[order[q][k]], dz,
        )

    def w_send(q, k, start):
        size = n >> (k + 1)
        b = bit[order[q][k]]
        away, kept = start + (1 - b) * size, start + b * size
        for j in range(size):
            wsend[q, offset[k] + j] = part[q, away + j].astype(BF16)
        go(w_copy(q, k))
        return kept

    def w_begin(q, grads):
        product = tn(layer[...], grads)
        for r in range(n):
            s = place(r, q)
            part[q, r] = product[s * z.rows_seq : (s + 1) * z.rows_seq, :]
        return w_send(q, 0, 0)

    def w_step(q, k, start):
        w_copy(q, k).wait_recv()
        size = n >> (k + 1)
        for j in range(size):
            part[q, start + j] += wrecv[q, offset[k] + j].astype(F32)
        if k + 1 < z.bits:
            return w_send(q, k + 1, start)
        scale = 1.0 / (pkcol[pl.ds(pl.multiple_of(me * z.rows_seq, 8), z.rows_seq), :] + EPSILON)
        value = part[q, start] * scale
        for d in range(m):
            piece = value[d * z.rows : (d + 1) * z.rows, :]
            zsend[q, d] = piece.astype(BF16)
            zown[q, d] = piece
        for o in range(1, m):
            go(z_copy(q, o))
        return start

    def z_copy(q, o):
        to = lax.rem(dz + o, m)
        return remote(
            zsend.at[q, to], zrecv.at[q, o - 1], zsem_s.at[q, o - 1], zsem_r.at[q, o - 1], me, to
        )

    def w_end(q):
        value = zown[q, dz]
        for o in range(1, m):
            z_copy(q, o).wait_recv()
            value += zrecv[q, o - 1].astype(F32)
        weight_out[:, q * states : (q + 1) * states] = value

    locals_[3].wait()
    grad_read = nn(mixed, writes) + nn(wcot[...], entry[...])
    reads_grad = (grad_read * slope[:, states:]).astype(BF16)
    grad_out[:, states:] = reads_grad
    at_read = w_begin(1, reads_grad)

    top = peak[...]
    for o in range(1, n):
        top = jnp.maximum(top, peak_recv[o - 1].astype(F32))
    peak_send2[...] = top.astype(BF16)
    peak_copies2 = [
        go(remote(peak_send2, peak_recv2.at[o - 1], qsem_s.at[o - 1], qsem_r.at[o - 1],
                  me, lax.rem(dz + o, m)))
        for o in range(1, m)
    ]

    def carried(half, c, state):
        width = z.chunk_rows
        at = pl.multiple_of(half * (z.channels // 2) + c * width, LANES)
        return nn(win[:, pl.ds(at, width)], state)

    for c in range(z.chunks):
        grad_write += carried(mine, c, beyond[c])
    for c in range(z.chunks):
        b_copies[c].wait_recv()
        grad_write += carried(other, c, brecv[c])
    writes_grad = (grad_write * slope[:, :states]).astype(BF16)
    grad_out[:, :states] = writes_grad
    at_write = w_begin(0, writes_grad)

    for o in range(1, m):
        peak_copies2[o - 1].wait_recv()
        top = jnp.maximum(top, peak_recv2[o - 1].astype(F32))
    unit = jnp.where(
        lax.broadcasted_iota(jnp.int32, (LANES, LANES), 0)
        == lax.broadcasted_iota(jnp.int32, (LANES, LANES), 1), 1.0, 0.0,
    ).astype(BF16)
    turned = nt(unit, top.astype(BF16))
    for j in range(z.wide):
        pkcol[j * LANES : (j + 1) * LANES, :] = jnp.broadcast_to(
            turned[:, j : j + 1], (LANES, LANES)
        )

    for k in range(z.bits):
        at_read = w_step(1, k, at_read)
        at_write = w_step(0, k, at_write)
    w_end(1)
    w_end(0)
    for copy in started:
        copy.wait_send()


def solution(mesh):
    n_seq, n_dp = mesh.shape["seq"], mesh.shape["dp"]

    def on_device(
        layer_input, scan_input, scan_cotangent, step_size, log_decay, state_inputs, entry_state
    ):
        tokens, width = layer_input.shape[1:]
        channels, heads = scan_input.shape[2], step_size.shape[1]
        states = state_inputs.shape[2] // 2
        z = Sizes(n_seq, n_dp, tokens, width, channels, heads, states)
        dma = pltpu.SemaphoreType.DMA
        chunk = (z.chunks, z.chunk_rows, states)
        steps_w = n_seq - 1
        peers, mates = max(n_dp - 1, 1), max(n_seq - 1, 1)
        peak = (z.wide_pad, LANES)
        block = (z.rows_seq, states)
        piece = (z.rows, states)
        V = pltpu.VMEM
        scratch = [
            V((tokens, width), BF16), V((tokens, channels), BF16), V((tokens, channels), BF16),
            V((channels, states), BF16), dma((4,)),
            V((heads, tokens), F32), V((heads, tokens, LANES), F32),
            V((heads, tokens, LANES), F32), V((tokens, channels), BF16),
            V((tokens, channels), BF16),
            V((z.bits,) + chunk, BF16), V((z.bits,) + chunk, BF16), V(chunk, F32), V(chunk, F32),
            V(chunk, F32), V(chunk, F32), V((z.bits, z.half_heads, LANES), F32),
            V((z.bits, z.half_heads, LANES), F32), V(chunk, BF16), V(chunk, BF16), V(chunk, BF16),
            dma((z.bits, z.chunks)), dma((z.bits, z.chunks)), dma((z.bits,)), dma((z.bits,)),
            dma((z.chunks,)), dma((z.chunks,)),
            V((tokens, tokens), F32), V((2, n_seq) + block, F32),
            V((2, steps_w) + block, BF16), V((2, steps_w) + block, BF16),
            dma((2, z.bits)), dma((2, z.bits)),
            V((2, n_dp) + piece, BF16), V((2, peers) + piece, BF16), V((2, n_dp) + piece, F32),
            dma((2, peers)), dma((2, peers)),
            V(peak, F32), V(peak, BF16), V((mates,) + peak, BF16), V(peak, BF16),
            V((peers,) + peak, BF16), V((width, LANES), F32),
            dma((mates,)), dma((mates,)), dma((peers,)), dma((peers,)),
        ]
        any_ = pl.BlockSpec(memory_space=pl.ANY)
        vmem = pl.BlockSpec(memory_space=pltpu.VMEM)
        grads, weights = pl.pallas_call(
            functools.partial(kernel, z),
            out_shape=(
                jax.ShapeDtypeStruct((tokens, 2 * states), BF16),
                jax.ShapeDtypeStruct((z.rows, 2 * states), F32),
            ),
            in_specs=[any_] * 4 + [vmem] * 3,
            out_specs=(vmem, vmem),
            scratch_shapes=scratch,
            compiler_params=pltpu.CompilerParams(
                collective_id=0, has_side_effects=True, vmem_limit_bytes=60 * 1024 * 1024
            ),
        )(
            layer_input[0], scan_input[0], scan_cotangent[0], entry_state[0, 0],
            step_size[0], log_decay[0], state_inputs[0],
        )
        return grads[None], weights

    placed = (
        P("dp", "seq", None),
        P("dp", "seq", None),
        P("dp", "seq", None),
        P("dp", None, "seq"),
        P("dp", None, "seq"),
        P("dp", "seq", None),
        P("dp", "seq", None, None),
    )
    return jax.shard_map(
        on_device,
        mesh=mesh,
        in_specs=placed,
        out_specs=(P("dp", "seq", None), P(("seq", "dp"), None)),
        check_vma=False,
    )
```

```python
import functools
import math

import jax
import jax.numpy as jnp
from jax import lax
from jax.experimental import pallas as pl
from jax.experimental.pallas import tpu as pltpu
from jax.sharding import PartitionSpec as P

MESH = pl.DeviceIdType.MESH
F32 = jnp.float32
BF16 = jnp.bfloat16
LANES = 128
LOG2E = 1.4426950408889634
EPSILON = 1e-06


def nt(a, b):
    return lax.dot_general(
        a, b, (((1,), (1,)), ((), ())), preferred_element_type=F32
    )


def tn(a, b):
    return lax.dot_general(a, b, (((0,), (0,)), ((), ())), preferred_element_type=F32)


def nn(a, b):
    return jnp.dot(a, b, preferred_element_type=F32)


class Sizes:
    def __init__(self, n_seq, n_dp, tokens, width, channels, heads, states):
        self.n_seq, self.n_dp, self.tokens, self.width = n_seq, n_dp, tokens, width
        self.channels, self.heads, self.states = channels, heads, states
        self.head = channels // heads
        self.bits = n_seq.bit_length() - 1
        self.half_heads = heads // 2
        self.half_pairs = channels // LANES // 2
        self.per = LANES // self.head
        self.chunks = max(c for c in range(1, 6) if self.half_pairs % c == 0)
        self.chunk_pairs = self.half_pairs // self.chunks
        self.chunk_rows = self.chunk_pairs * LANES
        self.chunk_heads = self.chunk_rows // self.head
        self.wide = width // LANES
        self.wide_pad = -(-self.wide // 16) * 16
        self.rows_seq = width // n_seq
        self.rows = self.rows_seq // n_dp
        self.streams = 2 if n_dp % 2 == 0 else 1


def kernel(
    z,
    layer_hbm, scan_hbm, cot_hbm, entry_hbm, step_ref, decay_ref, state_ref,
    grad_out, weight_out,
    layer, scan, cot, entry, local_sem,
    crow, ccol, wcol, wcot, win,
    fsend, frecv, fown, fhigh, fsum, bsum, dsend, drecv, bsend, brecv,
    fsem_s, fsem_r, dsem_s, dsem_r, bsem_s, bsem_r,
    mix, layer_t, part, wsend, wrecv, wsem_s, wsem_r, zsend, zrecv, zown, zsem_s, zsem_r,
    peak, peak_send, peak_recv, peak_send2, peak_recv2, pkcol,
    psem_s, psem_r, qsem_s, qsem_r,
):
    n, m, t = z.n_seq, z.n_dp, z.tokens
    me, dz = lax.axis_index("seq"), lax.axis_index("dp")
    bit = [lax.rem(me // (1 << b), 2) for b in range(z.bits)]
    mate = [me + (1 - 2 * bit[b]) * (1 << b) for b in range(z.bits)]
    mine, other = bit[0], 1 - bit[0]

    locals_ = [
        pltpu.make_async_copy(src, dst, local_sem.at[i])
        for i, (src, dst) in enumerate(
            ((cot_hbm, cot), (scan_hbm, scan), (layer_hbm, layer), (entry_hbm, entry))
        )
    ]
    for c in locals_:
        c.start()

    barrier = pltpu.get_barrier_semaphore()
    for o in range(1, n):
        pl.semaphore_signal(
            barrier, inc=1, device_id={"seq": lax.rem(me + o, n), "dp": dz}, device_id_type=MESH
        )
    for o in range(1, m):
        pl.semaphore_signal(
            barrier, inc=1, device_id={"seq": me, "dp": lax.rem(dz + o, m)}, device_id_type=MESH
        )

    decay = decay_ref[...] * LOG2E
    row = lax.broadcasted_iota(jnp.int32, (t, t), 0)
    col = lax.broadcasted_iota(jnp.int32, (t, t), 1)
    lower = jnp.where(col <= row, 1.0, 0.0).astype(BF16)
    cum = cum_t = 0.0
    for _ in range(3):
        piece = decay.astype(BF16)
        decay = decay - piece.astype(F32)
        cum, cum_t = cum + nt(piece, lower), cum_t + nt(lower, piece)
    steps = step_ref[...]
    crow[...] = cum - jnp.log2(steps)
    weight_t = jnp.transpose(steps) * jnp.exp2(cum_t[t - 1 : t, :] - cum_t)
    lane = lax.broadcasted_iota(jnp.int32, (t, LANES), 1)
    total = jnp.broadcast_to(jnp.exp2(cum[:, t - 1 : t]), (z.heads, LANES))
    tot = [total[: z.half_heads], total[z.half_heads :]]
    tot_mine = jnp.where(mine == 1, tot[1], tot[0])
    dsend[0] = jnp.where(mine == 1, tot[0], tot[1])
    for h in range(z.heads):
        ccol[h] = jnp.broadcast_to(cum_t[:, h : h + 1], (t, LANES))

    pre = state_ref[...].astype(F32)
    sigma = 1.0 / (1.0 + jnp.exp(-pre))
    activated = (pre * sigma).astype(BF16)
    writes, reads = activated[:, : z.states], activated[:, z.states :]

    def by_head(g, table):
        value = table[g * z.per]
        for k in range(1, z.per):
            value = jnp.where(lane >= k * z.head, table[g * z.per + k], value)
        return value

    def later(g):
        at = pl.ds(pl.multiple_of(g * LANES, LANES), LANES)
        weighted = (cot[:, at].astype(F32) * jnp.exp2(by_head(g, ccol))).astype(BF16)
        wcot[:, at] = weighted
        return tn(weighted, reads)

    def remote(src, dst, s_sem, r_sem, seq, dp):
        return pltpu.make_async_remote_copy(
            src_ref=src, dst_ref=dst, send_sem=s_sem, recv_sem=r_sem,
            device_id={"seq": seq, "dp": dp}, device_id_type=MESH,
        )

    def f_copy(b, c):
        return remote(
            fsend.at[b, c], frecv.at[b, c], fsem_s.at[b, c], fsem_r.at[b, c], mate[b], dz
        )

    def d_copy(b):
        return remote(dsend.at[b], drecv.at[b], dsem_s.at[b], dsem_r.at[b], mate[b], dz)

    def spread(d, c):
        return jnp.concatenate(
            [
                jnp.broadcast_to(d[h : h + 1, :], (z.head, LANES))
                for h in range(c * z.chunk_heads, (c + 1) * z.chunk_heads)
            ],
            axis=0,
        )

    started = []

    def go(copy):
        copy.start()
        started.append(copy)
        return copy

    locals_[0].wait()
    for c in range(z.chunks):
        for p in range(z.chunk_pairs):
            g = other * z.half_pairs + c * z.chunk_pairs + p
            fsend[0, c, p * LANES : (p + 1) * LANES, :] = later(g).astype(BF16)
        if c == 0:
            pl.semaphore_wait(barrier, n - 1 + m - 1)
            go(d_copy(0))
        go(f_copy(0, c))
    for c in range(z.chunks):
        for p in range(z.chunk_pairs):
            g = mine * z.half_pairs + c * z.chunk_pairs + p
            fown[c, p * LANES : (p + 1) * LANES, :] = later(g)

    d_copy(0).wait_recv()
    tot_other = drecv[0]
    tot_low = jnp.where(mine == 1, tot_other, tot_mine)
    tot_high = jnp.where(mine == 1, tot_mine, tot_other)
    d_now = tot_low * tot_high
    if z.bits > 1:
        dsend[1] = d_now
        go(d_copy(1))
    for c in range(z.chunks):
        f_copy(0, c).wait_recv()
        own, far = fown[c], frecv[0, c].astype(F32)
        up = jnp.where(mine == 1, own, far)
        fhigh[c] = up
        value = jnp.where(mine == 1, far, own) + spread(tot_low, c) * up
        bsum[c] = jnp.zeros_like(value)
        fsum[c] = value
        if z.bits > 1:
            fsend[1, c] = value.astype(BF16)
            go(f_copy(1, c))

    locals_[2].wait()
    peak[...] = jnp.zeros_like(peak)
    for j in range(z.wide):
        block = layer[:, j * LANES : (j + 1) * LANES].astype(F32)
        peak[j : j + 1, :] = jnp.max(jnp.abs(block), axis=0, keepdims=True)
    peak_send[...] = peak[...].astype(BF16)
    peak_copies = [
        go(remote(peak_send, peak_recv.at[o - 1], psem_s.at[o - 1], psem_r.at[o - 1],
                  lax.rem(me + o, n), dz))
        for o in range(1, n)
    ]

    locals_[1].wait()
    for h in range(z.heads):
        wcol[h] = jnp.broadcast_to(weight_t[:, h : h + 1], (t, LANES))
    mix[...] = jnp.zeros_like(mix)
    hf = t // 2
    keep = row[:hf, :hf] >= col[:hf, :hf]

    def mixing(g, carry):
        at = pl.ds(pl.multiple_of(g * LANES, LANES), LANES)
        c_pair, s_pair = cot[:, at], scan[:, at]
        win[:, at] = (s_pair.astype(F32) * by_head(g, wcol)).astype(BF16)
        for k in range(z.per):
            h = g * z.per + k
            inside = (lane >= k * z.head) & (lane < (k + 1) * z.head)
            c_head = jnp.where(inside, c_pair.astype(F32), 0.0).astype(BF16)
            rows = crow[pl.ds(h, 1), :]
            for s in range(2):
                scores = nt(c_head[s * hf : (s + 1) * hf], s_pair[: (s + 1) * hf])
                for r in range(s + 1):
                    cols = ccol[h, s * hf : (s + 1) * hf, :]
                    cut = slice(r * hf, (r + 1) * hf)
                    spread_ = cols - rows[:, cut]
                    if s == r:
                        spread_ = jnp.where(keep, spread_, -1e30)
                    mix[s * hf : (s + 1) * hf, cut] += scores[:, cut] * jnp.exp2(spread_)
        return carry

    fills = [
        (i * (z.heads // z.per) // z.chunks, (i + 1) * (z.heads // z.per) // z.chunks)
        for i in range(z.chunks)
    ]

    def fill():
        if fills:
            lax.fori_loop(*fills.pop(0), mixing, 0)

    slope = sigma * (1.0 + pre * (1.0 - sigma))
    states, half = z.states, z.rows_seq // z.streams
    order = {}
    for q in range(2):
        for i in range(z.streams):
            rest = list(range(1, z.bits))
            order[q, i] = [0] + (rest[::-1] if q == 0 and i == 1 else rest)
    number = {key: i for i, key in enumerate(order)}
    offset = [sum(n >> (k + 1) for k in range(i)) for i in range(z.bits)]

    def spot(u, key):
        r = 0
        for b in order[key][1:]:
            r = 2 * r + ((u >> (b - 1)) & 1)
        return r

    def w_copy(key, k):
        at, w = pl.ds(offset[k], n >> (k + 1)), number[key]
        return remote(
            wsend.at[w, at], wrecv.at[w, at], wsem_s.at[w, k], wsem_r.at[w, k],
            mate[order[key][k]], dz,
        )

    def w_begin(q, grads):
        def block(u, low):
            s = 2 * u + low
            at = pl.ds(pl.multiple_of(s * z.rows_seq, 16), z.rows_seq)
            return nn(layer_t[at, :], grads)

        for u in range(n // 2):
            value = block(u, other).astype(BF16)
            for i in range(z.streams):
                wsend[number[q, i], spot(u, (q, i))] = value[i * half : (i + 1) * half]
        for i in range(z.streams):
            go(w_copy((q, i), 0))
        for u in range(n // 2):
            value = block(u, mine)
            for i in range(z.streams):
                part[number[q, i], spot(u, (q, i))] = value[i * half : (i + 1) * half]

    starts = {key: 0 for key in order}

    def w_step(key, k):
        w_copy(key, k).wait_recv()
        w, start = number[key], starts[key]
        size = n >> (k + 1)
        if k + 1 < z.bits:
            away_size = size // 2
            b = bit[order[key][k + 1]]
            away, kept = (1 - b) * away_size, b * away_size
            for j in range(away_size):
                value = part[w, start + away + j] + wrecv[w, offset[k] + away + j].astype(F32)
                wsend[w, offset[k + 1] + j] = value.astype(BF16)
            go(w_copy(key, k + 1))
            for j in range(away_size):
                part[w, start + kept + j] += wrecv[w, offset[k] + kept + j].astype(F32)
            starts[key] = start + kept
            return
        value = part[w, start] + wrecv[w, offset[k]].astype(F32)
        first = me * z.rows_seq + key[1] * half
        scale = 1.0 / (pkcol[pl.ds(pl.multiple_of(first, 8), half), :] + EPSILON)
        value = value * scale
        base, count = key[1] * m // z.streams, m // z.streams
        for d in range(count):
            piece = value[d * z.rows : (d + 1) * z.rows, :]
            zsend[key[0], base + d] = piece.astype(BF16)
            zown[key[0], base + d] = piece

    def z_copy(q, o):
        to = lax.rem(dz + o, m)
        return remote(
            zsend.at[q, to], zrecv.at[q, o - 1], zsem_s.at[q, o - 1], zsem_r.at[q, o - 1], me, to
        )

    def w_cross(q):
        for o in range(m - 1, 0, -1):
            go(z_copy(q, o))

    def w_end(q):
        value = zown[q, dz]
        for o in range(1, m):
            z_copy(q, o).wait_recv()
            value += zrecv[q, o - 1].astype(F32)
        weight_out[:, q * states : (q + 1) * states] = value

    acc = []
    b_copies = []

    def early():
        while fills:
            fill()
        top = peak[...]
        for o in range(1, n):
            peak_copies[o - 1].wait_recv()
            top = jnp.maximum(top, peak_recv[o - 1].astype(F32))
        peak_send2[...] = top.astype(BF16)
        peak_copies2 = [
            go(remote(peak_send2, peak_recv2.at[o - 1], qsem_s.at[o - 1], qsem_r.at[o - 1],
                      me, lax.rem(dz + o, m)))
            for o in range(1, m)
        ]
        mixed = mix[...].astype(BF16)
        acc.append(tn(mixed, reads))
        locals_[3].wait()
        grad_read = nn(mixed, writes) + nn(wcot[...], entry[...])
        reads_grad = (grad_read * slope[:, states:]).astype(BF16)
        grad_out[:, states:] = reads_grad
        layer_t[...] = jnp.transpose(layer[...])
        w_begin(1, reads_grad)
        for i in range(z.streams):
            w_step((1, i), 0)
        for o in range(1, m):
            peak_copies2[o - 1].wait_recv()
            top = jnp.maximum(top, peak_recv2[o - 1].astype(F32))
        unit = jnp.where(
            lax.broadcasted_iota(jnp.int32, (LANES, LANES), 0)
            == lax.broadcasted_iota(jnp.int32, (LANES, LANES), 1), 1.0, 0.0,
        ).astype(BF16)
        turned = nt(unit, top.astype(BF16))
        for j in range(z.wide):
            pkcol[j * LANES : (j + 1) * LANES, :] = jnp.broadcast_to(
                turned[:, j : j + 1], (LANES, LANES)
            )

    def carried(side, c, state):
        at = pl.multiple_of(side * (z.channels // 2) + c * z.chunk_rows, LANES)
        return nn(win[:, pl.ds(at, z.chunk_rows)], state)

    def finish(c, above):
        low = fhigh[c] + spread(tot_high, c) * above
        bsend[c] = jnp.where(mine == 1, low, above).astype(BF16)
        b_copies.append(
            go(remote(bsend.at[c], brecv.at[c], bsem_s.at[c], bsem_r.at[c], mate[0], dz))
        )
        acc[0] += carried(mine, c, jnp.where(mine == 1, above, low).astype(BF16))

    e_now = None
    for b in range(1, z.bits):
        last = b == z.bits - 1
        if last:
            early()
        d_copy(b).wait_recv()
        d_far = drecv[b]
        d_low = jnp.where(bit[b] == 1, d_far, d_now)
        if not last:
            dsend[b + 1] = d_now * d_far
            go(d_copy(b + 1))
        for c in range(z.chunks):
            f_copy(b, c).wait_recv()
            far = frecv[b, c].astype(F32)
            scaled = far if e_now is None else spread(e_now, c) * far
            gained = bsum[c] + jnp.where(bit[b] == 1, jnp.zeros_like(scaled), scaled)
            if last:
                finish(c, gained)
                continue
            bsum[c] = gained
            own = fsum[c]
            value = jnp.where(bit[b] == 1, far, own) + spread(d_low, c) * jnp.where(
                bit[b] == 1, own, far
            )
            fsum[c] = value
            fsend[b + 1, c] = value.astype(BF16)
            go(f_copy(b + 1, c))
            if b == 1:
                fill()
        one = jnp.ones_like(d_far) if e_now is None else e_now
        e_now = jnp.where(bit[b] == 1, one, one * d_far)
        d_now = d_now * d_far
    if z.bits == 1:
        early()
        for c in range(z.chunks):
            finish(c, bsum[c])

    keys = {q: [(q, i) for i in range(z.streams)] for q in range(2)}
    if z.bits > 1:
        for key in keys[1]:
            w_step(key, 1)
    grad_write = acc[0]
    for c in range(z.chunks):
        b_copies[c].wait_recv()
        grad_write += carried(other, c, brecv[c])
    writes_grad = (grad_write * slope[:, :states]).astype(BF16)
    w_begin(0, writes_grad)
    grad_out[:, :states] = writes_grad
    for k in range(z.bits):
        for key in keys[0]:
            w_step(key, k)
        if k + 1 == z.bits:
            w_cross(0)
        if k + 2 < z.bits:
            for key in keys[1]:
                w_step(key, k + 2)
        if k + 3 == z.bits or (k == 0 and z.bits < 3):
            w_cross(1)
    w_end(1)
    w_end(0)
    for copy in started:
        copy.wait_send()


def settle(grads, weights, grads_out, weights_out):
    grads_out[0] = grads[...]
    weights_out[...] = weights[...]


def solution(mesh):
    n_seq, n_dp = mesh.shape["seq"], mesh.shape["dp"]

    def on_device(
        layer_input, scan_input, scan_cotangent, step_size, log_decay, state_inputs, entry_state
    ):
        tokens, width = layer_input.shape[1:]
        channels, heads = scan_input.shape[2], step_size.shape[1]
        states = state_inputs.shape[2] // 2
        z = Sizes(n_seq, n_dp, tokens, width, channels, heads, states)
        dma = pltpu.SemaphoreType.DMA
        chunk = (z.chunks, z.chunk_rows, states)
        steps_w, flows = n_seq - 1, 2 * z.streams
        peers, mates = max(n_dp - 1, 1), max(n_seq - 1, 1)
        peak = (z.wide_pad, LANES)
        block = (z.rows_seq // z.streams, states)
        piece = (z.rows, states)
        V = pltpu.VMEM
        scratch = [
            V((tokens, width), BF16), V((tokens, channels), BF16), V((tokens, channels), BF16),
            V((channels, states), BF16), dma((4,)),
            V((heads, tokens), F32), V((heads, tokens, LANES), F32),
            V((heads, tokens, LANES), F32), V((tokens, channels), BF16),
            V((tokens, channels), BF16),
            V((z.bits,) + chunk, BF16), V((z.bits,) + chunk, BF16), V(chunk, F32), V(chunk, F32),
            V(chunk, F32), V(chunk, F32), V((z.bits, z.half_heads, LANES), F32),
            V((z.bits, z.half_heads, LANES), F32), V(chunk, BF16), V(chunk, BF16),
            dma((z.bits, z.chunks)), dma((z.bits, z.chunks)), dma((z.bits,)), dma((z.bits,)),
            dma((z.chunks,)), dma((z.chunks,)),
            V((tokens, tokens), F32), V((width, tokens), BF16),
            V((flows, n_seq // 2) + block, F32),
            V((flows, steps_w) + block, BF16), V((flows, steps_w) + block, BF16),
            dma((flows, z.bits)), dma((flows, z.bits)),
            V((2, n_dp) + piece, BF16), V((2, peers) + piece, BF16), V((2, n_dp) + piece, F32),
            dma((2, peers)), dma((2, peers)),
            V(peak, F32), V(peak, BF16), V((mates,) + peak, BF16), V(peak, BF16),
            V((peers,) + peak, BF16), V((width, LANES), F32),
            dma((mates,)), dma((mates,)), dma((peers,)), dma((peers,)),
        ]
        any_ = pl.BlockSpec(memory_space=pl.ANY)
        vmem = pl.BlockSpec(memory_space=pltpu.VMEM)
        grads, weights = pl.pallas_call(
            functools.partial(kernel, z),
            out_shape=(
                jax.ShapeDtypeStruct((tokens, 2 * states), BF16),
                jax.ShapeDtypeStruct((z.rows, 2 * states), F32),
            ),
            in_specs=[any_] * 4 + [vmem] * 3,
            out_specs=(vmem, vmem),
            scratch_shapes=scratch,
            compiler_params=pltpu.CompilerParams(
                collective_id=0, has_side_effects=True, vmem_limit_bytes=60 * 1024 * 1024
            ),
        )(
            layer_input[0], scan_input[0], scan_cotangent[0], entry_state[0, 0],
            step_size[0], log_decay[0], state_inputs[0],
        )
        return pl.pallas_call(
            settle,
            out_shape=(
                jax.ShapeDtypeStruct((1,) + grads.shape, BF16),
                jax.ShapeDtypeStruct(weights.shape, F32),
            ),
            in_specs=[vmem, vmem],
            out_specs=(vmem, vmem),
        )(grads, weights)

    placed = (
        P("dp", "seq", None),
        P("dp", "seq", None),
        P("dp", "seq", None),
        P("dp", None, "seq"),
        P("dp", None, "seq"),
        P("dp", "seq", None),
        P("dp", "seq", None, None),
    )
    return jax.shard_map(
        on_device,
        mesh=mesh,
        in_specs=placed,
        out_specs=(P("dp", "seq", None), P(("seq", "dp"), None)),
        check_vma=False,
    )
```

```python
import functools
import math

import jax
import jax.numpy as jnp
from jax import lax
from jax.experimental import pallas as pl
from jax.experimental.pallas import tpu as pltpu
from jax.sharding import PartitionSpec as P

MESH = pl.DeviceIdType.MESH
F32 = jnp.float32
BF16 = jnp.bfloat16
LANES = 128
LOG2E = 1.4426950408889634
EPSILON = 1e-06


def nt(a, b):
    return lax.dot_general(
        a, b, (((1,), (1,)), ((), ())), preferred_element_type=F32
    )


def tn(a, b):
    return lax.dot_general(a, b, (((0,), (0,)), ((), ())), preferred_element_type=F32)


def nn(a, b):
    return jnp.dot(a, b, preferred_element_type=F32)


class Sizes:
    def __init__(self, n_seq, n_dp, tokens, width, channels, heads, states):
        self.n_seq, self.n_dp, self.tokens, self.width = n_seq, n_dp, tokens, width
        self.channels, self.heads, self.states = channels, heads, states
        self.head = channels // heads
        self.bits = n_seq.bit_length() - 1
        self.half_heads = heads // 2
        self.half_pairs = channels // LANES // 2
        self.per = LANES // self.head
        self.chunks = max(c for c in range(1, 6) if self.half_pairs % c == 0)
        self.chunk_pairs = self.half_pairs // self.chunks
        self.chunk_rows = self.chunk_pairs * LANES
        self.chunk_heads = self.chunk_rows // self.head
        self.wide = width // LANES
        self.wide_pad = -(-self.wide // 16) * 16
        self.rows_seq = width // n_seq
        self.rows = self.rows_seq // n_dp
        self.streams = 2 if n_dp % 2 == 0 else 1


def kernel(
    z,
    layer_hbm, scan_hbm, cot_hbm, entry_hbm, step_ref, decay_ref, state_ref,
    grad_out, weight_out,
    layer, scan, cot, entry, local_sem,
    crow, ccol, wcol, wcot, win,
    fsend, frecv, fown, fhigh, fsum, bsum, dsend, drecv, bsend, brecv,
    fsem_s, fsem_r, dsem_s, dsem_r, bsem_s, bsem_r,
    mix, layer_t, part, wsend, wrecv, wsem_s, wsem_r, zsend, zrecv, zown, zsem_s, zsem_r,
    peak, peak_send, peak_recv, peak_send2, peak_recv2, pkcol,
    psem_s, psem_r, qsem_s, qsem_r,
):
    n, m, t = z.n_seq, z.n_dp, z.tokens
    me, dz = lax.axis_index("seq"), lax.axis_index("dp")
    bit = [lax.rem(me // (1 << b), 2) for b in range(z.bits)]
    mate = [me + (1 - 2 * bit[b]) * (1 << b) for b in range(z.bits)]
    mine, other = bit[0], 1 - bit[0]

    locals_ = [
        pltpu.make_async_copy(src, dst, local_sem.at[i])
        for i, (src, dst) in enumerate(
            ((cot_hbm, cot), (scan_hbm, scan), (layer_hbm, layer), (entry_hbm, entry))
        )
    ]
    for c in locals_:
        c.start()

    barrier = pltpu.get_barrier_semaphore()
    for o in range(1, n):
        pl.semaphore_signal(
            barrier, inc=1, device_id={"seq": lax.rem(me + o, n), "dp": dz}, device_id_type=MESH
        )
    for o in range(1, m):
        pl.semaphore_signal(
            barrier, inc=1, device_id={"seq": me, "dp": lax.rem(dz + o, m)}, device_id_type=MESH
        )

    decay = decay_ref[...] * LOG2E
    row = lax.broadcasted_iota(jnp.int32, (t, t), 0)
    col = lax.broadcasted_iota(jnp.int32, (t, t), 1)
    lower = jnp.where(col <= row, 1.0, 0.0).astype(BF16)
    cum = cum_t = 0.0
    for _ in range(3):
        piece = decay.astype(BF16)
        decay = decay - piece.astype(F32)
        cum, cum_t = cum + nt(piece, lower), cum_t + nt(lower, piece)
    steps = step_ref[...]
    crow[...] = cum - jnp.log2(steps)
    weight_t = jnp.transpose(steps) * jnp.exp2(cum_t[t - 1 : t, :] - cum_t)
    lane = lax.broadcasted_iota(jnp.int32, (t, LANES), 1)
    total = jnp.broadcast_to(jnp.exp2(cum[:, t - 1 : t]), (z.heads, LANES))
    tot = [total[: z.half_heads], total[z.half_heads :]]
    tot_mine = jnp.where(mine == 1, tot[1], tot[0])
    dsend[0] = jnp.where(mine == 1, tot[0], tot[1])
    for h in range(z.heads):
        ccol[h] = jnp.broadcast_to(cum_t[:, h : h + 1], (t, LANES))

    pre = state_ref[...].astype(F32)
    sigma = 1.0 / (1.0 + jnp.exp(-pre))
    activated = (pre * sigma).astype(BF16)
    writes, reads = activated[:, : z.states], activated[:, z.states :]

    def by_head(g, table):
        value = table[g * z.per]
        for k in range(1, z.per):
            value = jnp.where(lane >= k * z.head, table[g * z.per + k], value)
        return value

    def later(g):
        at = pl.ds(pl.multiple_of(g * LANES, LANES), LANES)
        weighted = (cot[:, at].astype(F32) * jnp.exp2(by_head(g, ccol))).astype(BF16)
        wcot[:, at] = weighted
        return tn(weighted, reads)

    def remote(src, dst, s_sem, r_sem, seq, dp):
        return pltpu.make_async_remote_copy(
            src_ref=src, dst_ref=dst, send_sem=s_sem, recv_sem=r_sem,
            device_id={"seq": seq, "dp": dp}, device_id_type=MESH,
        )

    def f_copy(b, c):
        return remote(
            fsend.at[b, c], frecv.at[b, c], fsem_s.at[b, c], fsem_r.at[b, c], mate[b], dz
        )

    def d_copy(b):
        return remote(dsend.at[b], drecv.at[b], dsem_s.at[b], dsem_r.at[b], mate[b], dz)

    def spread(d, c):
        return jnp.concatenate(
            [
                jnp.broadcast_to(d[h : h + 1, :], (z.head, LANES))
                for h in range(c * z.chunk_heads, (c + 1) * z.chunk_heads)
            ],
            axis=0,
        )

    started = []

    def go(copy):
        copy.start()
        started.append(copy)
        return copy

    locals_[0].wait()
    for c in range(z.chunks):
        for p in range(z.chunk_pairs):
            g = other * z.half_pairs + c * z.chunk_pairs + p
            fsend[0, c, p * LANES : (p + 1) * LANES, :] = later(g).astype(BF16)
        if c == 0:
            pl.semaphore_wait(barrier, n - 1 + m - 1)
            go(d_copy(0))
        go(f_copy(0, c))
    for c in range(z.chunks):
        for p in range(z.chunk_pairs):
            g = mine * z.half_pairs + c * z.chunk_pairs + p
            fown[c, p * LANES : (p + 1) * LANES, :] = later(g)

    d_copy(0).wait_recv()
    tot_other = drecv[0]
    tot_low = jnp.where(mine == 1, tot_other, tot_mine)
    tot_high = jnp.where(mine == 1, tot_mine, tot_other)
    d_now = tot_low * tot_high
    if z.bits > 1:
        dsend[1] = d_now
        go(d_copy(1))
    for c in range(z.chunks):
        f_copy(0, c).wait_recv()
        own, far = fown[c], frecv[0, c].astype(F32)
        up = jnp.where(mine == 1, own, far)
        fhigh[c] = up
        value = jnp.where(mine == 1, far, own) + spread(tot_low, c) * up
        bsum[c] = jnp.zeros_like(value)
        fsum[c] = value
        if z.bits > 1:
            fsend[1, c] = value.astype(BF16)
            go(f_copy(1, c))

    locals_[2].wait()
    peak[...] = jnp.zeros_like(peak)
    for j in range(z.wide):
        block = layer[:, j * LANES : (j + 1) * LANES].astype(F32)
        peak[j : j + 1, :] = jnp.max(jnp.abs(block), axis=0, keepdims=True)
    peak_send[...] = peak[...].astype(BF16)
    peak_copies = [
        go(remote(peak_send, peak_recv.at[o - 1], psem_s.at[o - 1], psem_r.at[o - 1],
                  lax.rem(me + o, n), dz))
        for o in range(1, n)
    ]

    locals_[1].wait()
    for h in range(z.heads):
        wcol[h] = jnp.broadcast_to(weight_t[:, h : h + 1], (t, LANES))
    mix[...] = jnp.zeros_like(mix)
    hf = t // 2
    keep = row[:hf, :hf] >= col[:hf, :hf]

    def mixing(g, carry):
        at = pl.ds(pl.multiple_of(g * LANES, LANES), LANES)
        c_pair, s_pair = cot[:, at], scan[:, at]
        win[:, at] = (s_pair.astype(F32) * by_head(g, wcol)).astype(BF16)
        for k in range(z.per):
            h = g * z.per + k
            inside = (lane >= k * z.head) & (lane < (k + 1) * z.head)
            c_head = jnp.where(inside, c_pair.astype(F32), 0.0).astype(BF16)
            rows = crow[pl.ds(h, 1), :]
            for s in range(2):
                scores = nt(c_head[s * hf : (s + 1) * hf], s_pair[: (s + 1) * hf])
                for r in range(s + 1):
                    cols = ccol[h, s * hf : (s + 1) * hf, :]
                    cut = slice(r * hf, (r + 1) * hf)
                    spread_ = cols - rows[:, cut]
                    if s == r:
                        spread_ = jnp.where(keep, spread_, -1e30)
                    mix[s * hf : (s + 1) * hf, cut] += scores[:, cut] * jnp.exp2(spread_)
        return carry

    fills = [
        (i * (z.heads // z.per) // z.chunks, (i + 1) * (z.heads // z.per) // z.chunks)
        for i in range(z.chunks)
    ]

    def fill():
        if fills:
            lax.fori_loop(*fills.pop(0), mixing, 0)

    slope = sigma * (1.0 + pre * (1.0 - sigma))
    states, half = z.states, z.rows_seq // z.streams
    order = {}
    for q in range(2):
        for i in range(z.streams):
            rest = list(range(1, z.bits))
            order[q, i] = [0] + (rest[::-1] if q == 0 and i == 1 else rest)
    number = {key: i for i, key in enumerate(order)}
    offset = [sum(n >> (k + 1) for k in range(i)) for i in range(z.bits)]

    def spot(u, key):
        r = 0
        for b in order[key][1:]:
            r = 2 * r + ((u >> (b - 1)) & 1)
        return r

    def w_copy(key, k):
        at, w = pl.ds(offset[k], n >> (k + 1)), number[key]
        return remote(
            wsend.at[w, at], wrecv.at[w, at], wsem_s.at[w, k], wsem_r.at[w, k],
            mate[order[key][k]], dz,
        )

    def w_begin(q, grads):
        def block(u, low):
            s = 2 * u + low
            at = pl.ds(pl.multiple_of(s * z.rows_seq, 16), z.rows_seq)
            return nn(layer_t[at, :], grads)

        for u in range(n // 2):
            value = block(u, other).astype(BF16)
            for i in range(z.streams):
                wsend[number[q, i], spot(u, (q, i))] = value[i * half : (i + 1) * half]
        for i in range(z.streams):
            go(w_copy((q, i), 0))
        for u in range(n // 2):
            value = block(u, mine)
            for i in range(z.streams):
                part[number[q, i], spot(u, (q, i))] = value[i * half : (i + 1) * half]

    starts = {key: 0 for key in order}

    def w_step(key, k):
        w_copy(key, k).wait_recv()
        w, start = number[key], starts[key]
        size = n >> (k + 1)
        if k + 1 < z.bits:
            away_size = size // 2
            b = bit[order[key][k + 1]]
            away, kept = (1 - b) * away_size, b * away_size
            for j in range(away_size):
                value = part[w, start + away + j] + wrecv[w, offset[k] + away + j].astype(F32)
                wsend[w, offset[k + 1] + j] = value.astype(BF16)
            go(w_copy(key, k + 1))
            for j in range(away_size):
                part[w, start + kept + j] += wrecv[w, offset[k] + kept + j].astype(F32)
            starts[key] = start + kept
            return
        value = part[w, start] + wrecv[w, offset[k]].astype(F32)
        first = me * z.rows_seq + key[1] * half
        scale = 1.0 / (pkcol[pl.ds(pl.multiple_of(first, 8), half), :] + EPSILON)
        value = value * scale
        base, count = key[1] * m // z.streams, m // z.streams
        for d in range(count):
            piece = value[d * z.rows : (d + 1) * z.rows, :]
            zsend[key[0], base + d] = piece.astype(BF16)
            zown[key[0], base + d] = piece

    def z_copy(q, o):
        to = lax.rem(dz + o, m)
        return remote(
            zsend.at[q, to], zrecv.at[q, o - 1], zsem_s.at[q, o - 1], zsem_r.at[q, o - 1], me, to
        )

    def w_cross(q):
        for o in range(m - 1, 0, -1):
            go(z_copy(q, o))

    def w_end(q):
        value = zown[q, dz]
        for o in range(1, m):
            z_copy(q, o).wait_recv()
            value += zrecv[q, o - 1].astype(F32)
        weight_out[:, q * states : (q + 1) * states] = value

    acc, tops = [], []
    b_copies = []

    def early():
        while fills:
            fill()
        top = peak[...]
        for o in range(1, n):
            peak_copies[o - 1].wait_recv()
            top = jnp.maximum(top, peak_recv[o - 1].astype(F32))
        tops.append(top)
        peak_send2[...] = top.astype(BF16)
        for o in range(1, m):
            tops.append(
                go(remote(peak_send2, peak_recv2.at[o - 1], qsem_s.at[o - 1], qsem_r.at[o - 1],
                          me, lax.rem(dz + o, m)))
            )
        mixed = mix[...].astype(BF16)
        acc.append(tn(mixed, reads))
        locals_[3].wait()
        grad_read = nn(mixed, writes) + nn(wcot[...], entry[...])
        reads_grad = (grad_read * slope[:, states:]).astype(BF16)
        grad_out[:, states:] = reads_grad
        layer_t[...] = jnp.transpose(layer[...])
        w_begin(1, reads_grad)

    def forward():
        for i in range(z.streams):
            w_step((1, i), 0)

    def columns():
        top = tops[0]
        for o in range(1, m):
            tops[o].wait_recv()
            top = jnp.maximum(top, peak_recv2[o - 1].astype(F32))
        unit = jnp.where(
            lax.broadcasted_iota(jnp.int32, (LANES, LANES), 0)
            == lax.broadcasted_iota(jnp.int32, (LANES, LANES), 1), 1.0, 0.0,
        ).astype(BF16)
        turned = nt(unit, top.astype(BF16))
        for j in range(z.wide):
            pkcol[j * LANES : (j + 1) * LANES, :] = jnp.broadcast_to(
                turned[:, j : j + 1], (LANES, LANES)
            )

    def carried(side, c, state):
        at = pl.multiple_of(side * (z.channels // 2) + c * z.chunk_rows, LANES)
        return nn(win[:, pl.ds(at, z.chunk_rows)], state)

    def finish(c, above):
        low = fhigh[c] + spread(tot_high, c) * above
        bsend[c] = jnp.where(mine == 1, low, above).astype(BF16)
        b_copies.append(
            go(remote(bsend.at[c], brecv.at[c], bsem_s.at[c], bsem_r.at[c], mate[0], dz))
        )
        acc[0] += carried(mine, c, jnp.where(mine == 1, above, low).astype(BF16))

    e_now = None
    for b in range(1, z.bits):
        last = b == z.bits - 1
        if last:
            early()
        d_copy(b).wait_recv()
        d_far = drecv[b]
        d_low = jnp.where(bit[b] == 1, d_far, d_now)
        if not last:
            dsend[b + 1] = d_now * d_far
            go(d_copy(b + 1))
        for c in range(z.chunks):
            f_copy(b, c).wait_recv()
            far = frecv[b, c].astype(F32)
            scaled = far if e_now is None else spread(e_now, c) * far
            gained = bsum[c] + jnp.where(bit[b] == 1, jnp.zeros_like(scaled), scaled)
            if last:
                finish(c, gained)
                if c == z.chunks // 2:
                    forward()
                continue
            bsum[c] = gained
            own = fsum[c]
            value = jnp.where(bit[b] == 1, far, own) + spread(d_low, c) * jnp.where(
                bit[b] == 1, own, far
            )
            fsum[c] = value
            fsend[b + 1, c] = value.astype(BF16)
            go(f_copy(b + 1, c))
            if b == 1:
                fill()
        one = jnp.ones_like(d_far) if e_now is None else e_now
        e_now = jnp.where(bit[b] == 1, one, one * d_far)
        d_now = d_now * d_far
    if z.bits == 1:
        early()
        for c in range(z.chunks):
            finish(c, bsum[c])
        forward()

    keys = {q: [(q, i) for i in range(z.streams)] for q in range(2)}
    grad_write = acc[0]
    for c in range(z.chunks):
        b_copies[c].wait_recv()
        grad_write += carried(other, c, brecv[c])
    writes_grad = (grad_write * slope[:, :states]).astype(BF16)
    w_begin(0, writes_grad)
    grad_out[:, :states] = writes_grad
    for k in range(z.bits):
        if k + 1 == z.bits and k == 0:
            columns()
        for key in keys[0]:
            w_step(key, k)
        if k == 0 and z.bits > 1:
            columns()
        if k + 1 == z.bits:
            w_cross(0)
        if k + 1 < z.bits:
            for key in keys[1]:
                w_step(key, k + 1)
        if k + 2 == z.bits or z.bits == 1:
            w_cross(1)
    w_end(1)
    w_end(0)
    for copy in started:
        copy.wait_send()


def settle(grads, weights, grads_out, weights_out):
    grads_out[0] = grads[...]
    weights_out[...] = weights[...]


def solution(mesh):
    n_seq, n_dp = mesh.shape["seq"], mesh.shape["dp"]

    def on_device(
        layer_input, scan_input, scan_cotangent, step_size, log_decay, state_inputs, entry_state
    ):
        tokens, width = layer_input.shape[1:]
        channels, heads = scan_input.shape[2], step_size.shape[1]
        states = state_inputs.shape[2] // 2
        z = Sizes(n_seq, n_dp, tokens, width, channels, heads, states)
        dma = pltpu.SemaphoreType.DMA
        chunk = (z.chunks, z.chunk_rows, states)
        steps_w, flows = n_seq - 1, 2 * z.streams
        peers, mates = max(n_dp - 1, 1), max(n_seq - 1, 1)
        peak = (z.wide_pad, LANES)
        block = (z.rows_seq // z.streams, states)
        piece = (z.rows, states)
        V = pltpu.VMEM
        scratch = [
            V((tokens, width), BF16), V((tokens, channels), BF16), V((tokens, channels), BF16),
            V((channels, states), BF16), dma((4,)),
            V((heads, tokens), F32), V((heads, tokens, LANES), F32),
            V((heads, tokens, LANES), F32), V((tokens, channels), BF16),
            V((tokens, channels), BF16),
            V((z.bits,) + chunk, BF16), V((z.bits,) + chunk, BF16), V(chunk, F32), V(chunk, F32),
            V(chunk, F32), V(chunk, F32), V((z.bits, z.half_heads, LANES), F32),
            V((z.bits, z.half_heads, LANES), F32), V(chunk, BF16), V(chunk, BF16),
            dma((z.bits, z.chunks)), dma((z.bits, z.chunks)), dma((z.bits,)), dma((z.bits,)),
            dma((z.chunks,)), dma((z.chunks,)),
            V((tokens, tokens), F32), V((width, tokens), BF16),
            V((flows, n_seq // 2) + block, F32),
            V((flows, steps_w) + block, BF16), V((flows, steps_w) + block, BF16),
            dma((flows, z.bits)), dma((flows, z.bits)),
            V((2, n_dp) + piece, BF16), V((2, peers) + piece, BF16), V((2, n_dp) + piece, F32),
            dma((2, peers)), dma((2, peers)),
            V(peak, F32), V(peak, BF16), V((mates,) + peak, BF16), V(peak, BF16),
            V((peers,) + peak, BF16), V((width, LANES), F32),
            dma((mates,)), dma((mates,)), dma((peers,)), dma((peers,)),
        ]
        any_ = pl.BlockSpec(memory_space=pl.ANY)
        vmem = pl.BlockSpec(memory_space=pltpu.VMEM)
        grads, weights = pl.pallas_call(
            functools.partial(kernel, z),
            out_shape=(
                jax.ShapeDtypeStruct((tokens, 2 * states), BF16),
                jax.ShapeDtypeStruct((z.rows, 2 * states), F32),
            ),
            in_specs=[any_] * 4 + [vmem] * 3,
            out_specs=(vmem, vmem),
            scratch_shapes=scratch,
            compiler_params=pltpu.CompilerParams(
                collective_id=0, has_side_effects=True, vmem_limit_bytes=60 * 1024 * 1024
            ),
        )(
            layer_input[0], scan_input[0], scan_cotangent[0], entry_state[0, 0],
            step_size[0], log_decay[0], state_inputs[0],
        )
        return pl.pallas_call(
            settle,
            out_shape=(
                jax.ShapeDtypeStruct((1,) + grads.shape, BF16),
                jax.ShapeDtypeStruct(weights.shape, F32),
            ),
            in_specs=[vmem, vmem],
            out_specs=(vmem, vmem),
        )(grads, weights)

    placed = (
        P("dp", "seq", None),
        P("dp", "seq", None),
        P("dp", "seq", None),
        P("dp", None, "seq"),
        P("dp", None, "seq"),
        P("dp", "seq", None),
        P("dp", "seq", None, None),
    )
    return jax.shard_map(
        on_device,
        mesh=mesh,
        in_specs=placed,
        out_specs=(P("dp", "seq", None), P(("seq", "dp"), None)),
        check_vma=False,
    )
```
